256 devices in a mesh: tm: 16 (over x_lo, y, core), strip: 16 (over z, x_hi).
Axes of the slice: x: 4 (x_hi: 2, x_lo: 2; x = x_hi * 2 + x_lo), y: 4, z: 8, core: 2. Of those that a mesh axis runs over, the one named last changes fastest.
Arguments:
- signal: bfloat16 [2, 64, 16384], P(None, 'strip', 'tm'), may hold values from -5 to 5
Outputs:
- spectrum: bfloat16 [2, 256, 64, 16, 1024], P(None, 'strip', None, 'tm')
The draws below stay inside these ranges and needn't reach their ends.
All inputs are finite; a program needn't handle non-finite values.
Results may differ from the reference program's by a relative error of at most 0.0069.
Values may be sent and summed in bfloat16 or wider, within the bound.
A program may use at most 64 MiB of HBM per device.

```python
import math
import jax
import jax.numpy as jnp
from jax import lax

K = 256
L = 16384
W = 64
NRES = 16
LB = 1024


def shard_levels(rng, shape, pieces, least, high):
    level = 1.0
    for axis_at, parts in pieces:
        draws = jax.random.uniform(jax.random.fold_in(jax.random.fold_in(rng, 6), axis_at), (parts,), jnp.float32, least / len(pieces), high / len(pieces))
        level = level * jnp.repeat(jnp.exp(draws), shape[axis_at] // parts).reshape((-1,) + (1,) * (len(shape) - 1 - axis_at))
    return level


def bell_draw(key, dims, deviation, bound, cuts=(), kind=jnp.bfloat16):
    result = deviation * jax.random.normal(key, dims, jnp.float32)
    if cuts:
        result = result * shard_levels(key, dims, cuts, -0.22, 0.18)
    return jnp.clip(result, -bound, bound).astype(kind)


def setup_inputs(seed: int = 0) -> dict:
    splits = jax.random.split(jax.random.key(seed), 2)
    return {
        "signal": bell_draw(splits[0], (2, W, L), 0.7, 5.0, ((1, 16), (2, 16))),
    }


TWO_PI = 2.0 * math.pi

def channel_filters(channel_ids, length):
    offsets = jnp.arange(length, dtype=jnp.int32)
    phases = channel_ids[:, None] * offsets[None, :] % length
    angles = jnp.float32(TWO_PI) * phases.astype(jnp.float32) / length
    hamming = 0.54 - 0.46 * jnp.cos(jnp.float32(TWO_PI) * offsets.astype(jnp.float32) / length)
    scaled = hamming[None, :] / math.sqrt(length)
    cosine = scaled * jnp.cos(angles)
    sine = scaled * jnp.sin(angles)
    real_rows = jnp.stack([cosine, sine], axis=1)
    imag_rows = jnp.stack([-sine, cosine], axis=1)
    return jnp.concatenate([real_rows, imag_rows], axis=0).astype(jnp.bfloat16)

def dft_pair(first, second, modulus, norm):
    phases = first[:, None] * second[None, :] % modulus
    angles = jnp.float32(TWO_PI) * phases.astype(jnp.float32) / modulus
    return (jnp.cos(angles) * norm, jnp.sin(angles) * norm)

def reference(signal):
    filters = channel_filters(jnp.arange(K, dtype=jnp.int32), K).astype(jnp.float32)
    res_ids = jnp.arange(NRES, dtype=jnp.int32)
    blk_ids = jnp.arange(LB, dtype=jnp.int32)
    small_cos, small_sin = dft_pair(res_ids, res_ids, NRES, 1.0 / math.sqrt(NRES))
    small_cos = small_cos.astype(jnp.bfloat16).astype(jnp.float32)
    small_sin = small_sin.astype(jnp.bfloat16).astype(jnp.float32)
    big_cos, big_sin = dft_pair(blk_ids, blk_ids, LB, 1.0 / math.sqrt(LB))
    big_cos = big_cos.astype(jnp.bfloat16).astype(jnp.float32)
    big_sin = big_sin.astype(jnp.bfloat16).astype(jnp.float32)
    twid_cos, twid_sin = dft_pair(res_ids, blk_ids, L, 1.0)
    high = lax.Precision.HIGHEST

    def one_window(window):
        extended = jnp.concatenate([window, jnp.zeros((2, K), jnp.bfloat16)], axis=1)
        wide = extended.astype(jnp.float32)[:, None, :]
        outcome = lax.conv_general_dilated(wide, filters, (1,), 'VALID', dimension_numbers=('CNH', 'OIH', 'CNH'), precision=high, preferred_element_type=jnp.float32)
        spectra = outcome[:, 0, :L].reshape(2, K, L)
        centered = wide[:, 0, K // 2:K // 2 + L]
        real_part = spectra[0] * centered[0][None, :] + spectra[1] * centered[1][None, :]
        imag_part = spectra[1] * centered[0][None, :] - spectra[0] * centered[1][None, :]
        products = jnp.stack([real_part, imag_part]).astype(jnp.bfloat16)
        products = lax.optimization_barrier(products).astype(jnp.float32).reshape(2, K, NRES, LB)
        section_real = jnp.einsum('qn,knm->kqm', small_cos, products[0], precision=high) + jnp.einsum('qn,knm->kqm', small_sin, products[1], precision=high)
        section_imag = jnp.einsum('qn,knm->kqm', small_cos, products[1], precision=high) - jnp.einsum('qn,knm->kqm', small_sin, products[0], precision=high)
        turned_real = section_real * twid_cos[None] + section_imag * twid_sin[None]
        turned_imag = section_imag * twid_cos[None] - section_real * twid_sin[None]
        partial_sums = jnp.stack([turned_real, turned_imag]).astype(jnp.bfloat16)
        partial_sums = lax.optimization_barrier(partial_sums).astype(jnp.float32)
        out_real = jnp.dot(partial_sums[0], big_cos, precision=high) + jnp.dot(partial_sums[1], big_sin, precision=high)
        out_imag = jnp.dot(partial_sums[1], big_cos, precision=high) - jnp.dot(partial_sums[0], big_sin, precision=high)
        return jnp.stack([out_real, out_imag]).astype(jnp.bfloat16)
    spectra_all = lax.map(one_window, jnp.transpose(signal, (1, 0, 2)))
    return jnp.transpose(spectra_all, (1, 2, 0, 3, 4))
```

```python
import functools
import math

import jax
import jax.numpy as jnp
import numpy as np
from jax import lax
from jax.experimental import pallas as pl
from jax.experimental.pallas import tpu as pltpu
from jax.sharding import PartitionSpec as P

K = 256
J = 64
L = 16384
NB = 16
NA = 16
NW = 64
LB = 1024
NCH = 16
LANES = 128
TH = 2.0 * math.pi / K
F32 = jnp.float32
BF16 = jnp.bfloat16


def np_bf16(x):
    return np.asarray(x, np.float32).astype(jnp.bfloat16)


def base_table():
    kap = np.arange(-1, NCH + 1)
    r = np.arange(K)
    ang = TH * ((r[:, None] * kap[None, :]) % K)
    c, s = np.cos(ang), np.sin(ang)
    t = np.zeros((4, 2, J, LANES))
    nk = NCH + 2
    t[:, 0, :, :nk] = c.reshape(4, J, nk)
    t[:, 1, :, :nk] = s.reshape(4, J, nk)
    t[:, 0, :, nk : 2 * nk] = -s.reshape(4, J, nk)
    t[:, 1, :, nk : 2 * nk] = c.reshape(4, J, nk)
    return np_bf16(t.reshape(4 * LANES, LANES))


def step_tables():
    nk = NCH + 2
    w = np.zeros((NCH // 2, 256, 2, 2, J))
    i = np.arange(J)[:, None]
    j = np.arange(J)[None, :]
    delta = j - i
    ham = (0.54 - 0.46 * np.cos(TH * delta)) / math.sqrt(K) * (delta > 0)
    jj = np.arange(J)
    for k in range(NCH):
        kp, kk = divmod(k, 2)
        gr = ham * np.cos(TH * k * delta)
        gi = ham * np.sin(TH * k * delta)
        w[kp, :J, kk, 0] = gr
        w[kp, :J, kk, 1] = gi
        w[kp, J : 2 * J, kk, 0] = -gi
        w[kp, J : 2 * J, kk, 1] = gr
        for off, coef in ((-1, -0.23), (0, 0.54), (1, -0.23)):
            kap = k + off
            co = coef / math.sqrt(K)
            row = LANES + kap + 1
            w[kp, row, kk, 0] = co * np.cos(TH * kap * jj)
            w[kp, row, kk, 1] = co * np.sin(TH * kap * jj)
            w[kp, row + nk, kk, 0] = -co * np.sin(TH * kap * jj)
            w[kp, row + nk, kk, 1] = co * np.cos(TH * kap * jj)
    return np_bf16(w.reshape(NCH // 2, 256, 256))


def dft_table():
    b = np.arange(LB)
    ang = 2.0 * math.pi * ((b[:, None] * b[None, :]) % LB) / LB
    return np_bf16(np.concatenate([np.cos(ang), np.sin(ang)], axis=0) / math.sqrt(LB))


def swap(x):
    return pltpu.roll(x, J, 1)


def body(xg, mod, pc, ps, tr, wt, cs, out, y32, yb, lhs, va, vb, sr, si):
    left = lax.broadcasted_iota(jnp.int32, (1, LANES), 1) < J
    sign = jnp.where(left, -1.0, 1.0).astype(F32)
    mc = mod[0:1, :]
    ms = mod[1:2, :]

    def load_windows(i, carry):
        s = i // NA
        a = i % NA
        for w in range(4):
            x = xg[s, a, w].astype(F32)
            y = x * mc + swap(x) * ms
            y32[pl.ds(a * (NB * NW) + s * 4 + w, NB, stride=NW), :] = y
        return carry

    lax.fori_loop(0, 16 * NA, load_windows, 0)
    y32[pl.ds(NA * NB * NW, 4 * NW), :] = jnp.zeros((4 * NW, LANES), F32)

    def to_low(i, carry):
        rows = pl.ds(pl.multiple_of(i * 512, 512), 512)
        yb[rows, :] = y32[rows, :].astype(BF16)
        return carry

    lax.fori_loop(0, 32, to_low, 0)
    yb[pl.ds(NA * NB * NW, 4 * NW), :] = jnp.zeros((4 * NW, LANES), BF16)

    def pair_step(g, carry):
        for e in range(2):

            def prep(a, c2):
                rho = a * NB + 2 * g + e
                r0 = pl.multiple_of(rho * NW, NW)
                dst = pl.ds(pl.multiple_of(a * NW, NW), NW)
                d = y32[pl.ds(r0 + 4 * NW, NW), :] - y32[pl.ds(r0, NW), :]
                lhs[e, dst, 0:LANES] = d.astype(BF16)
                y2 = y32[pl.ds(r0 + 2 * NW, NW), :]
                v = y2 * pc[pl.ds(rho, 1), :] + swap(y2) * ps[pl.ds(rho, 1), :]
                va[e, dst, :] = v
                vb[e, dst, :] = swap(v) * sign
                return c2

            lax.fori_loop(0, NA, prep, 0)
            for h in range(4):
                parts = []
                for a4 in range(4):
                    r0 = ((h * 4 + a4) * NB + 2 * g + e) * NW
                    parts.append(
                        jnp.concatenate(
                            [yb[pl.ds(pl.multiple_of(r0 + q * NW, NW), NW), :] for q in range(4)],
                            axis=1,
                        )
                    )
                rows = jnp.concatenate(parts, axis=0)
                base = jnp.dot(rows, tr[...], preferred_element_type=F32)
                lhs[e, h * 256 : (h + 1) * 256, LANES:] = base.astype(BF16)

        lane0 = pl.multiple_of(g * LANES, LANES)

        def chan_step(kp, c2):
            w = wt[kp]
            got = []
            for e in range(2):
                x = jnp.dot(lhs[e], w, preferred_element_type=F32)
                ta = [jnp.zeros((NW, LANES), F32) for _ in range(2)]
                tb = [jnp.zeros((NW, LANES), F32) for _ in range(2)]
                for a in range(NA):
                    rows = slice(a * NW, (a + 1) * NW)
                    ua = va[e, rows, :]
                    ub = vb[e, rows, :]
                    for kk in range(2):
                        xa = x[rows, kk * LANES : (kk + 1) * LANES]
                        ta[kk] = ta[kk] + xa * ua
                        tb[kk] = tb[kk] + xa * ub
                got.append(([t + swap(t) for t in ta], [t + swap(t) for t in tb]))
            for kk in range(2):
                re = jnp.where(left, got[0][0][kk], got[1][0][kk])
                im = jnp.where(left, got[0][1][kk], got[1][1][kk])
                sr[2 * kp + kk, :, pl.ds(lane0, LANES)] = re.astype(BF16)
                si[2 * kp + kk, :, pl.ds(lane0, LANES)] = im.astype(BF16)
            return c2

        lax.fori_loop(0, NCH // 2, chan_step, 0)
        return carry

    lax.fori_loop(0, NB // 2, pair_step, 0)

    def finish(k, carry):
        re = sr[k]
        im = si[k]
        both = jnp.concatenate(
            [jnp.concatenate([re, im], axis=1), jnp.concatenate([im, -re], axis=1)], axis=0
        )
        z = jnp.dot(both, cs[...], preferred_element_type=F32).astype(BF16)
        out[0, k] = z[:NW]
        out[1, k] = z[NW:]
        return carry

    lax.fori_loop(0, NCH, finish, 0)


def compute(xg, mod, pc, ps):
    vm = pl.BlockSpec(memory_space=pltpu.VMEM)
    return pl.pallas_call(
        body,
        out_shape=jax.ShapeDtypeStruct((2, NCH, NW, LB), BF16),
        in_specs=[vm] * 7,
        out_specs=vm,
        scratch_shapes=[
            pltpu.VMEM(((NA * NB + 4) * NW, LANES), F32),
            pltpu.VMEM(((NA * NB + 4) * NW, LANES), BF16),
            pltpu.VMEM((2, NA * NW, 256), BF16),
            pltpu.VMEM((2, NA * NW, LANES), F32),
            pltpu.VMEM((2, NA * NW, LANES), F32),
            pltpu.VMEM((NCH, NW, LB), BF16),
            pltpu.VMEM((NCH, NW, LB), BF16),
        ],
        compiler_params=pltpu.CompilerParams(vmem_limit_bytes=60 * 2**20),
    )(xg, mod, pc, ps, jnp.asarray(base_table()), jnp.asarray(step_tables()), jnp.asarray(dft_table()))


def phases(s, p):
    lane = jnp.arange(LANES, dtype=jnp.int32)
    left = lane < J
    ang = jnp.float32(2.0 * math.pi / 16) * ((s * (lane % 16)) % 16).astype(F32)
    sm = jnp.sin(ang)
    mod = jnp.stack([jnp.cos(ang), jnp.where(left, sm, -sm)])
    n = jnp.arange(NA * NB, dtype=jnp.int32)[:, None] * J + (lane % J)[None, :]
    ang = jnp.float32(2.0 * math.pi / L) * ((p * n) % L).astype(F32)
    sp = 0.25 * jnp.sin(ang)
    return mod, 0.25 * jnp.cos(ang), jnp.where(left[None, :], -sp, sp)


def blocks_of(signal):
    four = signal.shape[1]
    return signal.reshape(2, four, NB, J).transpose(1, 2, 0, 3).reshape(four, NB, LANES)


def per_device(signal):
    mine = blocks_of(signal)
    xg = lax.all_gather(mine, ("strip", "tm")).reshape(16, NA, 4, NB, LANES)
    mod, pc, ps = phases(lax.axis_index("strip"), lax.axis_index("tm"))
    return compute(xg, mod, pc, ps).reshape(2, NCH, NW, 1, LB)


def solution(mesh):
    return jax.shard_map(
        per_device,
        mesh=mesh,
        in_specs=(P(None, "strip", "tm"),),
        out_specs=P(None, "strip", None, "tm", None),
        check_vma=False,
    )
```

```python
import math

import jax
import jax.numpy as jnp
import numpy as np
from jax import lax
from jax.experimental import pallas as pl
from jax.experimental.pallas import tpu as pltpu
from jax.sharding import PartitionSpec as P

K = 256
J = 64
L = 16384
NB = 16
NA = 16
NW = 64
LB = 1024
NCH = 16
LANES = 128
GW = 8
NZ = 8
KB = 4
QB = 4
TH = 2.0 * math.pi / K
F32 = jnp.float32
BF16 = jnp.bfloat16


ORDER = np.arange(J).reshape(J // 4, 4).T.reshape(J)


def np_bf16(x):
    return np.asarray(x, np.float32).astype(jnp.bfloat16)


def base_table():
    kap = np.arange(-1, NCH + 1)
    r = np.arange(K)
    ang = TH * ((r[:, None] * kap[None, :]) % K)
    c, s = np.cos(ang), np.sin(ang)
    t = np.zeros((4, 2, J, LANES))
    nk = NCH + 2
    c = c.reshape(4, J, nk)[:, ORDER]
    s = s.reshape(4, J, nk)[:, ORDER]
    t[:, 0, :, :nk] = c
    t[:, 1, :, :nk] = s
    t[:, 0, :, nk : 2 * nk] = -s
    t[:, 1, :, nk : 2 * nk] = c
    return np_bf16(t.reshape(4 * LANES, LANES))


def step_tables():
    nk = NCH + 2
    w = np.zeros((NCH // 2, 256, 2, 2, J))
    i = ORDER[:, None]
    j = ORDER[None, :]
    delta = j - i
    ham = (0.54 - 0.46 * np.cos(TH * delta)) / math.sqrt(K) * (delta > 0)
    jj = ORDER
    for k in range(NCH):
        kp, kk = divmod(k, 2)
        gr = ham * np.cos(TH * k * delta)
        gi = ham * np.sin(TH * k * delta)
        w[kp, :J, kk, 0] = gr
        w[kp, :J, kk, 1] = gi
        w[kp, J : 2 * J, kk, 0] = -gi
        w[kp, J : 2 * J, kk, 1] = gr
        for off, coef in ((-1, -0.23), (0, 0.54), (1, -0.23)):
            kap = k + off
            co = coef / math.sqrt(K)
            row = LANES + kap + 1
            w[kp, row, kk, 0] = co * np.cos(TH * kap * jj)
            w[kp, row, kk, 1] = co * np.sin(TH * kap * jj)
            w[kp, row + nk, kk, 0] = -co * np.sin(TH * kap * jj)
            w[kp, row + nk, kk, 1] = co * np.cos(TH * kap * jj)
    return np_bf16(w.reshape(NCH // 2, 256, 256))


def dft_tables():
    group = np.arange(2 * NB * LANES // 2) // 16
    tile, part = group // 8, group % 8
    blk = np.zeros(LB, np.int64)
    low = np.zeros(LB, np.int64)
    for n in range(LB):
        t, q = tile[n], part[n]
        bits = [q % 2, q // 2 % 2]
        low[n] = (t % 2) + 2 * (t // 2 % 2)
        src = (t // 4) * 4 + bits[0] + 2 * bits[1]
        blk[n] = 2 * src + q // 4
    b = blk * J + (np.arange(LB) % 16) * 4 + low
    m = np.arange(LB // 4)
    out = np.zeros((4, 2, LB // 4, 2, LB // 4))
    for r in range(4):
        rows = b[low == r]
        ang = 2.0 * math.pi * ((rows[:, None] * m[None, :]) % LB) / LB
        c, d = np.cos(ang) / math.sqrt(LB), np.sin(ang) / math.sqrt(LB)
        out[r, 0, :, 0] = c
        out[r, 0, :, 1] = -d
        out[r, 1, :, 0] = d
        out[r, 1, :, 1] = c
    return np_bf16(out.reshape(4, LB // 2, LB // 2))


def phase_tables():
    lane = np.arange(LANES)
    left = lane < J
    place = ORDER[lane % J]
    ids = np.arange(16)
    ang = 2.0 * math.pi * ((ids[:, None] * place[None, :]) % 16) / 16
    mod = np.zeros((16, 8, LANES), np.float32)
    mod[:, 0] = np.cos(ang)
    mod[:, 1] = np.where(left, np.sin(ang), -np.sin(ang))
    ang = 2.0 * math.pi * ids[:, None] * place[None, :] / L
    turn = np.zeros((16, 8, LANES), np.float32)
    turn[:, 0] = 0.25 * np.cos(ang)
    turn[:, 1] = 0.25 * np.sin(ang)
    turn[:, 2] = 0.25 * np.where(left, -np.cos(ang), np.cos(ang))
    turn[:, 3] = 0.25 * np.where(left, -np.sin(ang), np.sin(ang))
    ang = np.broadcast_to(2.0 * math.pi * np.arange(K)[:, None] / K, (K, LANES))
    circle = np.stack([np.cos(ang), np.sin(ang)]).astype(np.float32)
    return mod, turn, circle


def pick_table():
    t = np.zeros((2, J, 2, J))
    for lane, j in enumerate(ORDER):
        t[0, j, 0, lane] = 1
        t[1, j, 1, lane] = 1
    return np_bf16(t.reshape(2, J, LANES))


def swap(x):
    return pltpu.roll(x, J, 1)


MESH = pl.DeviceIdType.MESH


def exchange_parts(mine, g, sems):
    (loc, ts, tr_, xs, xr, rs, rr, ls, lr, ds, dr) = sems
    t = lax.axis_index("tm")
    s = lax.axis_index("strip")
    core = t % 2
    q = t // 2
    z = s // 2
    sib = t + 1 - 2 * core
    other = s + 1 - 2 * (s % 2)

    def ring(z_from, e, h, right):
        ref = g.at[2 * z_from + e, core]
        to = (2 * ((z + 1) % NZ) if right else 2 * ((z + NZ - 1) % NZ)) + s % 2
        send, recv = (rs, rr) if right else (ls, lr)
        return pltpu.make_async_remote_copy(
            src_ref=ref,
            dst_ref=ref,
            send_sem=send.at[h, e],
            recv_sem=recv.at[h, e],
            device_id={"strip": to},
            device_id_type=MESH,
        )

    def twin(strip, half, slot):
        ref = g.at[strip, half]
        return pltpu.make_async_remote_copy(
            src_ref=ref,
            dst_ref=ref,
            send_sem=ds.at[slot],
            recv_sem=dr.at[slot],
            device_id={"tm": sib},
            device_id_type=MESH,
        )

    def far(d, half, pos):
        ref = g.at[s, half, pos]
        return pltpu.make_async_remote_copy(
            src_ref=ref,
            dst_ref=ref,
            send_sem=ts.at[d],
            recv_sem=tr_.at[d],
            device_id={"tm": (t + d) % NA},
            device_id_type=MESH,
        )

    def cross(strip):
        ref = g.at[strip, core]
        return pltpu.make_async_remote_copy(
            src_ref=ref,
            dst_ref=ref,
            send_sem=xs,
            recv_sem=xr,
            device_id={"strip": other},
            device_id_type=MESH,
        )

    def slot_of(e, h, right):
        return 1 + (h * 2 + e) * 2 + (0 if right else 1)

    def begin():
        local = pltpu.make_async_copy(mine, g.at[s, core, q], loc)
        local.start()
        barrier = pltpu.get_barrier_semaphore()
        for d in range(1, NA):
            pl.semaphore_signal(barrier, inc=1, device_id={"tm": (t + d) % NA}, device_id_type=MESH)
        for to in (other, 2 * ((z + 1) % NZ) + s % 2, 2 * ((z + NZ - 1) % NZ) + s % 2):
            pl.semaphore_signal(barrier, inc=1, device_id={"strip": to}, device_id_type=MESH)
        pl.semaphore_wait(barrier, NA - 1 + 3)
        local.wait()
        for d in range(1, NA):
            far(d, core, q).start()

    def joined():
        for d in range(1, NA):
            src = (t + NA - d) % NA
            far(d, src % 2, src // 2).wait_recv()
        cross(s).start()
        ring(z, s % 2, 1, True).start()
        ring(z, s % 2, 1, False).start()

    def open_partner():
        cross(other).wait_recv()
        twin(other, core, 0).start()
        ring(z, other % 2, 1, True).start()
        ring(z, other % 2, 1, False).start()
        twin(other, 1 - core, 0).wait_recv()

    def arrive(h, e, right, last=False):
        zf = (z + NZ - h) % NZ if right else (z + h) % NZ
        ring(zf, e, h, right).wait_recv()
        twin(2 * zf + e, core, slot_of(e, h, right)).start()

        if not last:
            if e == (0 if right else 1):
                ring(zf, e, h + 1, right).start()
            else:

                @pl.when(h < 3)
                def _():
                    ring(zf, e, h + 1, right).start()

    def settle(h, e, right):
        zf = (z + NZ - h) % NZ if right else (z + h) % NZ
        twin(2 * zf + e, 1 - core, slot_of(e, h, right)).wait_recv()

    def close():
        for d in range(1, NA):
            far(d, core, q).wait_send()
        cross(s).wait_send()
        twin(other, core, 0).wait_send()
        for right in (True, False):
            for h in range(1, 5):
                for e in range(2):
                    if h == 4 and e != (0 if right else 1):
                        continue
                    zs = (z + NZ - h + 1) % NZ if right else (z + h - 1) % NZ
                    zf = (z + NZ - h) % NZ if right else (z + h) % NZ
                    ring(zs, e, h, right).wait_send()
                    twin(2 * zf + e, core, slot_of(e, h, right)).wait_send()

    return z, begin, joined, open_partner, arrive, settle, close


def body(mine, mod_h, turn_h, circle_h, tr_h, wt_h, sr_h, si_h, g, mod, turn, circle, tr, wt, pce, pse, y32, yb, lhs, va, vb, sr, si, fl, tab, *sems):
    z0, begin, joined, open_partner, arrive, settle, close = exchange_parts(mine, g, sems)
    pairs = ((mod_h.at[lax.axis_index("strip")], mod), (turn_h.at[lax.axis_index("tm")], turn), (circle_h, circle), (tr_h, tr), (wt_h, wt))
    tables = [pltpu.make_async_copy(h, v, tab.at[i]) for i, (h, v) in enumerate(pairs)]
    for c in tables:
        c.start()
    begin()
    left = lax.broadcasted_iota(jnp.int32, (1, LANES), 1) < J
    sign = jnp.where(left, -1.0, 1.0).astype(F32)
    rows_all = NA * NB * GW
    tables[0].wait()
    tables[1].wait()
    mc = mod[0:1, :]
    ms = mod[1:2, :]

    tables[2].wait()
    me = lax.axis_index("tm")
    turns = [jnp.broadcast_to(turn[i : i + 1, :], (GW, LANES)) for i in range(4)]

    def spread(rho, carry):
        at = (me * rho) % K
        ca = jnp.broadcast_to(circle[0, pl.ds(at, 1), :], (GW, LANES))
        sa = jnp.broadcast_to(circle[1, pl.ds(at, 1), :], (GW, LANES))
        dst = pl.ds(pl.multiple_of(rho * GW, GW), GW)
        pce[dst, :] = ca * turns[0] - sa * turns[1]
        pse[dst, :] = sa * turns[2] + ca * turns[3]
        return carry

    lax.fori_loop(0, NA * NB, spread, 0, unroll=8)
    y32[pl.ds(rows_all, 4 * GW), :] = jnp.zeros((4 * GW, LANES), F32)
    yb[pl.ds(rows_all, 4 * GW), :] = jnp.zeros((4 * GW, LANES), BF16)

    joined()
    tables[3].wait()
    tables[4].wait()
    open_partner()

    def flush(z):
        return [pltpu.make_async_copy(v.at[:, z], h.at[:, z], fl.at[z, n]) for n, (v, h) in enumerate(((sr, sr_h), (si, si_h)))]

    def group(i, carry):
        half = (i + 1) // 2
        z = (z0 + NZ + half * (1 - 2 * (i % 2))) % NZ

        @pl.when(i % 2 == 1)
        def _():
            @pl.when(half < 4)
            def _():
                for e in range(2):
                    for right in (True, False):
                        arrive(half, e, right)
                for e in range(2):
                    settle(half, e, True)

            @pl.when(half == 4)
            def _():
                arrive(half, 0, True, True)
                arrive(half, 1, False, True)
                settle(half, 0, True)
                settle(half, 1, False)

        @pl.when((i % 2 == 0) & (i > 0))
        def _():
            for e in range(2):
                settle(half, e, False)

        def load_windows(a, c2):
            for xh in range(2):
                for w in range(4):
                    x = g[2 * z + xh, a % 2, a // 2, w].astype(F32)
                    y = x * mc + swap(x) * ms
                    y32[pl.ds(a * (NB * GW) + xh * 4 + w, NB, stride=GW), :] = y
            return c2

        lax.fori_loop(0, NA, load_windows, 0, unroll=4)

        step = 256
        count = rows_all // step
        for i in range(count + 1):
            if i < count:
                r0 = i * step
                rows = slice(r0, r0 + step)
                y = y32[rows, :]
                yb[rows, :] = y.astype(BF16)
                d = y32[r0 + 4 * GW : r0 + 4 * GW + step, :] - y
                lhs[rows, 0:LANES] = d.astype(BF16)
                y2 = y32[r0 + 2 * GW : r0 + 2 * GW + step, :]
                v = y2 * pce[rows, :] + swap(y2) * pse[rows, :]
                va[rows, :] = v
                vb[rows, :] = swap(v) * sign
            if i > 0:
                r0 = (i - 1) * step
                rows = jnp.concatenate([yb[r0 + q * GW : r0 + q * GW + step, :] for q in range(4)], axis=1)
                base = jnp.dot(rows, tr[...], preferred_element_type=F32)
                lhs[r0 : r0 + step, LANES:] = base.astype(BF16)

        def chan_step(kp, c2):
            w = wt[kp]
            for qb in range(NB // QB):
                cuts = [slice((a * NB + qb * QB) * GW, (a * NB + (qb + 1) * QB) * GW) for a in range(NA)]
                x = jnp.dot(
                    jnp.concatenate([lhs[c, :] for c in cuts], axis=0), w, preferred_element_type=F32
                )
                n = QB * GW
                ta = [None] * 2
                tb = [None] * 2
                for a in range(NA):
                    ua = va[cuts[a], :]
                    ub = vb[cuts[a], :]
                    for kk in range(2):
                        xa = x[a * n : (a + 1) * n, kk * LANES : (kk + 1) * LANES]
                        ta[kk] = xa * ua if a == 0 else ta[kk] + xa * ua
                        tb[kk] = xa * ub if a == 0 else tb[kk] + xa * ub
                for kk in range(2):
                    for t, dst in ((ta[kk], sr), (tb[kk], si)):
                        t = t + swap(t)
                        for h in range(QB // 2):
                            even = t[2 * h * GW : (2 * h + 1) * GW]
                            odd = t[(2 * h + 1) * GW : (2 * h + 2) * GW]
                            lane0 = (qb * QB // 2 + h) * LANES
                            dst[2 * kp + kk, z, :, lane0 : lane0 + LANES] = jnp.where(left, even, odd).astype(BF16)
            return c2

        lax.fori_loop(0, NCH // 2, chan_step, 0, unroll=4)
        for c in flush(z):
            c.start()
        return carry

    lax.fori_loop(0, NW // GW, group, 0)
    for z in range(NZ):
        for c in flush(z):
            c.wait()

    close()


def last_pass(sr, si, tab, out, acc):
    lane = lax.broadcasted_iota(jnp.int32, (1, LANES), 1)
    n = KB * NW

    def regroup(ref):
        t = [ref[:, :, :, i * LANES : (i + 1) * LANES].reshape(n, LANES).astype(F32) for i in range(8)]
        for bit in range(2):
            sh = 16 << bit
            low = (lane // sh) % 2 == 0
            for i in range(8):
                if i >> bit & 1:
                    continue
                p, q = t[i], t[i + (1 << bit)]
                t[i] = jnp.where(low, p, pltpu.roll(q, sh, 1))
                t[i + (1 << bit)] = jnp.where(low, pltpu.roll(p, LANES - sh, 1), q)
        return [x.astype(BF16) for x in t]

    re = regroup(sr)
    im = regroup(si)
    for r in range(4):
        rows = jnp.concatenate([re[r], re[r + 4], im[r], im[r + 4]], axis=1)
        acc[r] = jnp.dot(rows, tab[r], preferred_element_type=F32)
    h = LB // 4
    for c0 in range(0, h, LANES):
        y = [(acc[r, :, c0 : c0 + LANES], acc[r, :, h + c0 : h + c0 + LANES]) for r in range(4)]
        for c in range(2):
            o = 1 - c
            sg = 1.0 if c == 0 else -1.0
            e0 = y[0][c] + y[2][c]
            e1 = y[0][c] - y[2][c]
            o0 = y[1][c] + y[3][c]
            o1 = (y[1][o] - y[3][o]) * sg
            for m1, val in enumerate((e0 + o0, e1 + o1, e0 - o0, e1 - o1)):
                lane0 = m1 * h + c0
                out[c, :, :, lane0 : lane0 + LANES] = val.astype(BF16).reshape(KB, NW, LANES)


def finish(sr, si):
    part = pl.BlockSpec((KB, NW // GW, GW, LB), lambda k: (k, 0, 0, 0))
    return pl.pallas_call(
        last_pass,
        grid=(NCH // KB,),
        out_shape=jax.ShapeDtypeStruct((2, NCH, NW, LB), BF16),
        in_specs=[part, part, pl.BlockSpec((4, LB // 2, LB // 2), lambda k: (0, 0, 0))],
        out_specs=pl.BlockSpec((2, KB, NW, LB), lambda k: (0, k, 0, 0)),
        scratch_shapes=[pltpu.VMEM((4, KB * NW, LB // 2), F32)],
        compiler_params=pltpu.CompilerParams(vmem_limit_bytes=67043328),
    )(sr, si, jnp.asarray(dft_tables()))


def compute(mine):
    hbm = pl.BlockSpec(memory_space=pltpu.HBM)
    dma = pltpu.SemaphoreType.DMA
    rows = NA * NB * GW
    mod, turn, circle = phase_tables()
    strip = jax.ShapeDtypeStruct((NCH, NW // GW, GW, LB), BF16)
    return pl.pallas_call(
        body,
        out_shape=(strip, strip),
        in_specs=[hbm] * 6,
        out_specs=(hbm, hbm),
        scratch_shapes=[
            pltpu.VMEM((2 * NZ, 2, NA // 2, 4, NB, LANES), BF16),
            pltpu.VMEM((8, LANES), F32),
            pltpu.VMEM((8, LANES), F32),
            pltpu.VMEM((2, K, LANES), F32),
            pltpu.VMEM((4 * LANES, LANES), BF16),
            pltpu.VMEM((NCH // 2, 256, 256), BF16),
            pltpu.VMEM((rows, LANES), F32),
            pltpu.VMEM((rows, LANES), F32),
            pltpu.VMEM((rows + 4 * GW, LANES), F32),
            pltpu.VMEM((rows + 4 * GW, LANES), BF16),
            pltpu.VMEM((rows, 256), BF16),
            pltpu.VMEM((rows, LANES), F32),
            pltpu.VMEM((rows, LANES), F32),
            pltpu.VMEM((NCH, NW // GW, GW, LB), BF16),
            pltpu.VMEM((NCH, NW // GW, GW, LB), BF16),
            dma((NZ, 2)),
            dma((5,)),
            dma,
            dma((NA,)),
            dma((NA,)),
            dma,
            dma,
            dma((5, 2)),
            dma((5, 2)),
            dma((5, 2)),
            dma((5, 2)),
            dma((21,)),
            dma((21,)),
        ],
        compiler_params=pltpu.CompilerParams(
            vmem_limit_bytes=67043328, collective_id=0, has_side_effects=True
        ),
    )(mine, jnp.asarray(mod), jnp.asarray(turn), jnp.asarray(circle), jnp.asarray(base_table()), jnp.asarray(step_tables()))


def blocks_of(signal):
    four = signal.shape[1]
    cut = signal.reshape(2, four, NB, J)
    return jnp.einsum("cwbj,cjl->wbl", cut, jnp.asarray(pick_table()), preferred_element_type=F32).astype(BF16)


def per_device(signal):
    sr, si = compute(blocks_of(signal))
    return finish(sr, si).reshape(2, NCH, NW, 1, LB)


def solution(mesh):
    return jax.shard_map(
        per_device,
        mesh=mesh,
        in_specs=(P(None, "strip", "tm"),),
        out_specs=P(None, "strip", None, "tm", None),
        check_vma=False,
    )
```

```python
import math

import jax
import jax.numpy as jnp
import numpy as np
from jax import lax
from jax.experimental import pallas as pl
from jax.experimental.pallas import tpu as pltpu
from jax.sharding import PartitionSpec as P

K = 256
J = 64
L = 16384
NB = 16
NA = 16
NW = 64
LB = 1024
NCH = 16
LANES = 128
GW = 8
NZ = 8
NQ = 8
KB = 4
QB = 4
TH = 2.0 * math.pi / K
F32 = jnp.float32
BF16 = jnp.bfloat16


ORDER = np.arange(J).reshape(J // 4, 4).T.reshape(J)


def np_bf16(x):
    return np.asarray(x, np.float32).astype(jnp.bfloat16)


def base_table():
    kap = np.arange(-1, NCH + 1)
    r = np.arange(K)
    ang = TH * ((r[:, None] * kap[None, :]) % K)
    c, s = np.cos(ang), np.sin(ang)
    t = np.zeros((4, 2, J, LANES))
    nk = NCH + 2
    c = c.reshape(4, J, nk)[:, ORDER]
    s = s.reshape(4, J, nk)[:, ORDER]
    t[:, 0, :, :nk] = c
    t[:, 1, :, :nk] = s
    t[:, 0, :, nk : 2 * nk] = -s
    t[:, 1, :, nk : 2 * nk] = c
    return np_bf16(t.reshape(4 * LANES, LANES))


def step_tables():
    nk = NCH + 2
    w = np.zeros((NCH // 2, 256, 2, 2, J))
    i = ORDER[:, None]
    j = ORDER[None, :]
    delta = j - i
    ham = (0.54 - 0.46 * np.cos(TH * delta)) / math.sqrt(K) * (delta > 0)
    jj = ORDER
    for k in range(NCH):
        kp, kk = divmod(k, 2)
        gr = ham * np.cos(TH * k * delta)
        gi = ham * np.sin(TH * k * delta)
        w[kp, :J, kk, 0] = gr
        w[kp, :J, kk, 1] = gi
        w[kp, J : 2 * J, kk, 0] = -gi
        w[kp, J : 2 * J, kk, 1] = gr
        for off, coef in ((-1, -0.23), (0, 0.54), (1, -0.23)):
            kap = k + off
            co = coef / math.sqrt(K)
            row = LANES + kap + 1
            w[kp, row, kk, 0] = co * np.cos(TH * kap * jj)
            w[kp, row, kk, 1] = co * np.sin(TH * kap * jj)
            w[kp, row + nk, kk, 0] = -co * np.sin(TH * kap * jj)
            w[kp, row + nk, kk, 1] = co * np.cos(TH * kap * jj)
    return np_bf16(w.reshape(NCH // 2, 256, 256))


def dft_tables():
    group = np.arange(2 * NB * LANES // 2) // 16
    tile, part = group // 8, group % 8
    blk = np.zeros(LB, np.int64)
    low = np.zeros(LB, np.int64)
    for n in range(LB):
        t, q = tile[n], part[n]
        bits = [q % 2, q // 2 % 2]
        low[n] = (t % 2) + 2 * (t // 2 % 2)
        src = (t // 4) * 4 + bits[0] + 2 * bits[1]
        blk[n] = 2 * src + q // 4
    b = blk * J + (np.arange(LB) % 16) * 4 + low
    m = np.arange(LB // 4)
    out = np.zeros((4, 2, LB // 4, 2, LB // 4))
    for r in range(4):
        rows = b[low == r]
        ang = 2.0 * math.pi * ((rows[:, None] * m[None, :]) % LB) / LB
        c, d = np.cos(ang) / math.sqrt(LB), np.sin(ang) / math.sqrt(LB)
        out[r, 0, :, 0] = c
        out[r, 0, :, 1] = -d
        out[r, 1, :, 0] = d
        out[r, 1, :, 1] = c
    return np_bf16(out.reshape(4, LB // 2, LB // 2))


def phase_tables():
    lane = np.arange(LANES)
    left = lane < J
    place = ORDER[lane % J]
    ids = np.arange(16)
    ang = 2.0 * math.pi * ((ids[:, None] * place[None, :]) % 16) / 16
    mod = np.zeros((16, 8, LANES), np.float32)
    mod[:, 0] = np.cos(ang)
    mod[:, 1] = np.where(left, np.sin(ang), -np.sin(ang))
    ang = 2.0 * math.pi * ids[:, None] * place[None, :] / L
    turn = np.zeros((16, 8, LANES), np.float32)
    turn[:, 0] = 0.25 * np.cos(ang)
    turn[:, 1] = 0.25 * np.sin(ang)
    turn[:, 2] = 0.25 * np.where(left, -np.cos(ang), np.cos(ang))
    turn[:, 3] = 0.25 * np.where(left, -np.sin(ang), np.sin(ang))
    ang = np.broadcast_to(2.0 * math.pi * np.arange(K)[:, None] / K, (K, LANES))
    circle = np.stack([np.cos(ang), np.sin(ang)]).astype(np.float32)
    return mod, turn, circle


def pick_table():
    t = np.zeros((2, 2, J, 2, 2, J))
    for lane, j in enumerate(ORDER):
        for c in range(2):
            for e in range(2):
                t[c, e, j, e, c, lane] = 1
    return np_bf16(t.reshape(256, 256))


def swap(x):
    return pltpu.roll(x, J, 1)


MESH = pl.DeviceIdType.MESH


def exchange_parts(g, sems):
    (ts, tr_, xs, xr, rs, rr, ls, lr, ds, dr) = sems
    t = lax.axis_index("tm")
    s = lax.axis_index("strip")
    core = t % 2
    q = t // 2
    z = s // 2
    sib = t + 1 - 2 * core
    other = s + 1 - 2 * (s % 2)
    up = 2 * ((z + 1) % NZ) + s % 2
    down = 2 * ((z + NZ - 1) % NZ) + s % 2

    def peer(d):
        return 2 * ((q + d) % NQ) + core

    def ring(z_from, e, h, right):
        ref = g.at[2 * z_from + e, core]
        send, recv = (rs, rr) if right else (ls, lr)
        return pltpu.make_async_remote_copy(
            src_ref=ref,
            dst_ref=ref,
            send_sem=send.at[h, e],
            recv_sem=recv.at[h, e],
            device_id={"strip": up if right else down},
            device_id_type=MESH,
        )

    def twin(strip, half, slot):
        ref = g.at[strip, half]
        return pltpu.make_async_remote_copy(
            src_ref=ref,
            dst_ref=ref,
            send_sem=ds.at[slot],
            recv_sem=dr.at[slot],
            device_id={"tm": sib},
            device_id_type=MESH,
        )

    def near(d, pos):
        ref = g.at[s, core, pos]
        return pltpu.make_async_remote_copy(
            src_ref=ref,
            dst_ref=ref,
            send_sem=ts.at[d],
            recv_sem=tr_.at[d],
            device_id={"tm": peer(d)},
            device_id_type=MESH,
        )

    def cross(d, strip, pos):
        ref = g.at[strip, core, pos]
        return pltpu.make_async_remote_copy(
            src_ref=ref,
            dst_ref=ref,
            send_sem=xs.at[d],
            recv_sem=xr.at[d],
            device_id={"strip": other, "tm": peer(d)},
            device_id_type=MESH,
        )

    def slot_of(e, h, right):
        return 2 + (h * 2 + e) * 2 + (0 if right else 1)

    def greet():
        barrier = pltpu.get_barrier_semaphore()
        ids = [{"tm": peer(d)} for d in range(1, NQ)]
        ids += [{"strip": other, "tm": peer(d)} for d in range(NQ)]
        ids += [{"tm": sib}, {"strip": up}, {"strip": down}]
        for to in ids:
            pl.semaphore_signal(barrier, inc=1, device_id=to, device_id_type=MESH)

    def begin(piece):
        g[s, core, q] = piece
        barrier = pltpu.get_barrier_semaphore()
        pl.semaphore_wait(barrier, 2 * NQ + 2)
        for d in range(NQ):
            cross(d, s, q).start()
            if d:
                near(d, q).start()

    def joined():
        for d in range(1, NQ):
            near(d, (q + NQ - d) % NQ).wait_recv()
        ring(z, s % 2, 1, True).start()
        ring(z, s % 2, 1, False).start()
        twin(s, core, 0).start()
        for d in range(NQ):
            cross(d, other, (q + NQ - d) % NQ).wait_recv()
        twin(other, core, 1).start()
        ring(z, other % 2, 1, True).start()
        ring(z, other % 2, 1, False).start()
        twin(s, 1 - core, 0).wait_recv()
        twin(other, 1 - core, 1).wait_recv()

    def arrive(h, e, right, last=False):
        zf = (z + NZ - h) % NZ if right else (z + h) % NZ
        ring(zf, e, h, right).wait_recv()
        twin(2 * zf + e, core, slot_of(e, h, right)).start()

        if not last:
            if e == (0 if right else 1):
                ring(zf, e, h + 1, right).start()
            else:

                @pl.when(h < 3)
                def _():
                    ring(zf, e, h + 1, right).start()

    def settle(h, e, right):
        zf = (z + NZ - h) % NZ if right else (z + h) % NZ
        twin(2 * zf + e, 1 - core, slot_of(e, h, right)).wait_recv()

    def close():
        for d in range(NQ):
            cross(d, s, q).wait_send()
            if d:
                near(d, q).wait_send()
        twin(s, core, 0).wait_send()
        twin(other, core, 1).wait_send()
        for right in (True, False):
            for h in range(1, 5):
                for e in range(2):
                    if h == 4 and e != (0 if right else 1):
                        continue
                    zs = (z + NZ - h + 1) % NZ if right else (z + h - 1) % NZ
                    zf = (z + NZ - h) % NZ if right else (z + h) % NZ
                    ring(zs, e, h, right).wait_send()
                    twin(2 * zf + e, core, slot_of(e, h, right)).wait_send()

    return z, greet, begin, joined, arrive, settle, close


def cut(x, pick):
    x = x.astype(F32)
    rows = []
    for n in range(NB // 2):
        both = jnp.concatenate([x[c][:, n * LANES : (n + 1) * LANES] for c in range(2)], axis=1)
        rows += [both, both]
    out = jnp.dot(jnp.concatenate(rows, axis=0).astype(BF16), pick, preferred_element_type=F32)
    low = lax.broadcasted_iota(jnp.int32, (4 * NB, LANES), 0) % 8 < 4
    return jnp.where(low, out[:, :LANES], out[:, LANES:]).astype(BF16)


def body(sig_h, pick_h, mod_h, turn_h, circle_h, tr_h, wt_h, sr_h, si_h, g, sig, pick, mod, turn, circle, tr, wt, pce, pse, y32, yb, lhs, va, vb, sr, si, fl, tab, *sems):
    z0, greet, begin, joined, arrive, settle, close = exchange_parts(g, sems)
    pairs = ((sig_h, sig), (pick_h, pick), (mod_h.at[lax.axis_index("strip")], mod), (turn_h.at[lax.axis_index("tm")], turn), (circle_h, circle), (tr_h, tr), (wt_h, wt))
    tables = [pltpu.make_async_copy(h, v, tab.at[i]) for i, (h, v) in enumerate(pairs)]
    for c in tables:
        c.start()
    greet()
    tables[0].wait()
    tables[1].wait()
    begin(cut(sig[...], pick[...]))
    left = lax.broadcasted_iota(jnp.int32, (1, LANES), 1) < J
    sign = jnp.where(left, -1.0, 1.0).astype(F32)
    rows_all = NA * NB * GW
    for c in tables[2:5]:
        c.wait()
    mc = mod[0:1, :]
    ms = mod[1:2, :]

    me = lax.axis_index("tm")
    turns = [jnp.broadcast_to(turn[i : i + 1, :], (GW, LANES)) for i in range(4)]

    def spread(rho, carry):
        at = (me * rho) % K
        ca = jnp.broadcast_to(circle[0, pl.ds(at, 1), :], (GW, LANES))
        sa = jnp.broadcast_to(circle[1, pl.ds(at, 1), :], (GW, LANES))
        dst = pl.ds(pl.multiple_of(rho * GW, GW), GW)
        pce[dst, :] = ca * turns[0] - sa * turns[1]
        pse[dst, :] = sa * turns[2] + ca * turns[3]
        return carry

    lax.fori_loop(0, NA * NB, spread, 0, unroll=8)
    y32[pl.ds(rows_all, 4 * GW), :] = jnp.zeros((4 * GW, LANES), F32)
    yb[pl.ds(rows_all, 4 * GW), :] = jnp.zeros((4 * GW, LANES), BF16)

    for c in tables[5:]:
        c.wait()
    joined()

    def flush(z):
        return [pltpu.make_async_copy(v.at[:, z], h.at[:, z], fl.at[z, n]) for n, (v, h) in enumerate(((sr, sr_h), (si, si_h)))]

    def group(i, carry):
        half = (i + 1) // 2
        z = (z0 + NZ + half * (1 - 2 * (i % 2))) % NZ

        @pl.when(i % 2 == 1)
        def _():
            @pl.when(half < 4)
            def _():
                for e in range(2):
                    for right in (True, False):
                        arrive(half, e, right)
                for e in range(2):
                    settle(half, e, True)

            @pl.when(half == 4)
            def _():
                arrive(half, 0, True, True)
                arrive(half, 1, False, True)
                settle(half, 0, True)
                settle(half, 1, False)

        @pl.when((i % 2 == 0) & (i > 0))
        def _():
            for e in range(2):
                settle(half, e, False)

        low = lax.broadcasted_iota(jnp.int32, (1, GW, LANES), 1) < 4

        def load_windows(a, c2):
            y = []
            for xh in range(2):
                x = g[2 * z + xh, a % 2, a // 2].astype(F32)
                y.append((x * mc + swap(x) * ms).reshape(NB // 2, GW, LANES))
            even = jnp.where(low, y[0], pltpu.roll(y[1], 4, 1))
            odd = jnp.where(low, pltpu.roll(y[0], 4, 1), y[1])
            both = jnp.stack([even, odd], axis=1).reshape(NB * GW, LANES)
            y32[pl.ds(pl.multiple_of(a * (NB * GW), NB * GW), NB * GW), :] = both
            return c2

        lax.fori_loop(0, NA, load_windows, 0, unroll=4)

        step = 256
        count = rows_all // step
        for i in range(count + 1):
            if i < count:
                r0 = i * step
                rows = slice(r0, r0 + step)
                y = y32[rows, :]
                yb[rows, :] = y.astype(BF16)
                d = y32[r0 + 4 * GW : r0 + 4 * GW + step, :] - y
                lhs[rows, 0:LANES] = d.astype(BF16)
                y2 = y32[r0 + 2 * GW : r0 + 2 * GW + step, :]
                v = y2 * pce[rows, :] + swap(y2) * pse[rows, :]
                va[rows, :] = v
                vb[rows, :] = swap(v) * sign
            if i > 0:
                r0 = (i - 1) * step
                rows = jnp.concatenate([yb[r0 + q * GW : r0 + q * GW + step, :] for q in range(4)], axis=1)
                base = jnp.dot(rows, tr[...], preferred_element_type=F32)
                lhs[r0 : r0 + step, LANES:] = base.astype(BF16)

        def chan_step(kp, c2):
            w = wt[kp]
            for qb in range(NB // QB):
                cuts = [slice((a * NB + qb * QB) * GW, (a * NB + (qb + 1) * QB) * GW) for a in range(NA)]
                x = jnp.dot(
                    jnp.concatenate([lhs[c, :] for c in cuts], axis=0), w, preferred_element_type=F32
                )
                n = QB * GW
                ta = [None] * 2
                tb = [None] * 2
                for a in range(NA):
                    ua = va[cuts[a], :]
                    ub = vb[cuts[a], :]
                    for kk in range(2):
                        xa = x[a * n : (a + 1) * n, kk * LANES : (kk + 1) * LANES]
                        ta[kk] = xa * ua if a == 0 else ta[kk] + xa * ua
                        tb[kk] = xa * ub if a == 0 else tb[kk] + xa * ub
                for kk in range(2):
                    for t, dst in ((ta[kk], sr), (tb[kk], si)):
                        t = t + swap(t)
                        for h in range(QB // 2):
                            even = t[2 * h * GW : (2 * h + 1) * GW]
                            odd = t[(2 * h + 1) * GW : (2 * h + 2) * GW]
                            lane0 = (qb * QB // 2 + h) * LANES
                            dst[2 * kp + kk, z, :, lane0 : lane0 + LANES] = jnp.where(left, even, odd).astype(BF16)
            return c2

        lax.fori_loop(0, NCH // 2, chan_step, 0, unroll=4)
        for c in flush(z):
            c.start()
        return carry

    lax.fori_loop(0, NW // GW, group, 0)
    for z in range(NZ):
        for c in flush(z):
            c.wait()

    close()


def last_pass(sr, si, tab, out, acc):
    lane = lax.broadcasted_iota(jnp.int32, (1, LANES), 1)
    n = KB * NW

    def regroup(ref):
        t = [ref[:, :, :, i * LANES : (i + 1) * LANES].reshape(n, LANES) for i in range(8)]
        for bit in range(2):
            sh = 16 << bit
            low = (lane // sh) % 2 == 0
            for i in range(8):
                if i >> bit & 1:
                    continue
                p, q = t[i], t[i + (1 << bit)]
                t[i] = jnp.where(low, p, pltpu.roll(q, sh, 1))
                t[i + (1 << bit)] = jnp.where(low, pltpu.roll(p, LANES - sh, 1), q)
        return t

    re = regroup(sr)
    im = regroup(si)
    for r in range(4):
        rows = jnp.concatenate([re[r], re[r + 4], im[r], im[r + 4]], axis=1)
        acc[r] = jnp.dot(rows, tab[r], preferred_element_type=F32)
    h = LB // 4
    for c0 in range(0, h, LANES):
        y = [(acc[r, :, c0 : c0 + LANES], acc[r, :, h + c0 : h + c0 + LANES]) for r in range(4)]
        for c in range(2):
            o = 1 - c
            sg = 1.0 if c == 0 else -1.0
            e0 = y[0][c] + y[2][c]
            e1 = y[0][c] - y[2][c]
            o0 = y[1][c] + y[3][c]
            o1 = (y[1][o] - y[3][o]) * sg
            for m1, val in enumerate((e0 + o0, e1 + o1, e0 - o0, e1 - o1)):
                lane0 = m1 * h + c0
                out[c, :, :, lane0 : lane0 + LANES] = val.astype(BF16).reshape(KB, NW, LANES)


def finish(sr, si):
    part = pl.BlockSpec((KB, NW // GW, GW, LB), lambda k: (k, 0, 0, 0))
    return pl.pallas_call(
        last_pass,
        grid=(NCH // KB,),
        out_shape=jax.ShapeDtypeStruct((2, NCH, NW, LB), BF16),
        in_specs=[part, part, pl.BlockSpec((4, LB // 2, LB // 2), lambda k: (0, 0, 0))],
        out_specs=pl.BlockSpec((2, KB, NW, LB), lambda k: (0, k, 0, 0)),
        scratch_shapes=[pltpu.VMEM((4, KB * NW, LB // 2), F32)],
        compiler_params=pltpu.CompilerParams(vmem_limit_bytes=67043328),
    )(sr, si, jnp.asarray(dft_tables()))


def compute(signal):
    hbm = pl.BlockSpec(memory_space=pltpu.HBM)
    dma = pltpu.SemaphoreType.DMA
    rows = NA * NB * GW
    mod, turn, circle = phase_tables()
    strip = jax.ShapeDtypeStruct((NCH, NW // GW, GW, LB), BF16)
    return pl.pallas_call(
        body,
        out_shape=(strip, strip),
        in_specs=[hbm] * 7,
        out_specs=(hbm, hbm),
        scratch_shapes=[
            pltpu.VMEM((2 * NZ, 2, NQ, 4 * NB, LANES), BF16),
            pltpu.VMEM((2, 4, LB), BF16),
            pltpu.VMEM((256, 256), BF16),
            pltpu.VMEM((8, LANES), F32),
            pltpu.VMEM((8, LANES), F32),
            pltpu.VMEM((2, K, LANES), F32),
            pltpu.VMEM((4 * LANES, LANES), BF16),
            pltpu.VMEM((NCH // 2, 256, 256), BF16),
            pltpu.VMEM((rows, LANES), F32),
            pltpu.VMEM((rows, LANES), F32),
            pltpu.VMEM((rows + 4 * GW, LANES), F32),
            pltpu.VMEM((rows + 4 * GW, LANES), BF16),
            pltpu.VMEM((rows, 256), BF16),
            pltpu.VMEM((rows, LANES), F32),
            pltpu.VMEM((rows, LANES), F32),
            pltpu.VMEM((NCH, NW // GW, GW, LB), BF16),
            pltpu.VMEM((NCH, NW // GW, GW, LB), BF16),
            dma((NZ, 2)),
            dma((7,)),
            dma((NQ,)),
            dma((NQ,)),
            dma((NQ,)),
            dma((NQ,)),
            dma((5, 2)),
            dma((5, 2)),
            dma((5, 2)),
            dma((5, 2)),
            dma((22,)),
            dma((22,)),
        ],
        compiler_params=pltpu.CompilerParams(
            vmem_limit_bytes=67043328, collective_id=0, has_side_effects=True
        ),
    )(signal, jnp.asarray(pick_table()), jnp.asarray(mod), jnp.asarray(turn), jnp.asarray(circle), jnp.asarray(base_table()), jnp.asarray(step_tables()))


def per_device(signal):
    sr, si = compute(signal)
    return finish(sr, si).reshape(2, NCH, NW, 1, LB)


def solution(mesh):
    return jax.shard_map(
        per_device,
        mesh=mesh,
        in_specs=(P(None, "strip", "tm"),),
        out_specs=P(None, "strip", None, "tm", None),
        check_vma=False,
    )
```

```python
import math

import jax
import jax.numpy as jnp
import numpy as np
from jax import lax
from jax.experimental import pallas as pl
from jax.experimental.pallas import tpu as pltpu
from jax.sharding import PartitionSpec as P

K = 256
J = 64
L = 16384
NB = 16
NA = 16
NW = 64
LB = 1024
NCH = 16
LANES = 128
GW = 8
NZ = 8
NQ = 8
KB = 4
QB = 4
TH = 2.0 * math.pi / K
F32 = jnp.float32
BF16 = jnp.bfloat16


ORDER = np.arange(J).reshape(J // 4, 4).T.reshape(J)


def np_bf16(x):
    return np.asarray(x, np.float32).astype(jnp.bfloat16)


def base_table():
    kap = np.arange(-1, NCH + 1)
    r = np.arange(K)
    ang = TH * ((r[:, None] * kap[None, :]) % K)
    c, s = np.cos(ang), np.sin(ang)
    t = np.zeros((4, 2, J, LANES))
    nk = NCH + 2
    c = c.reshape(4, J, nk)[:, ORDER]
    s = s.reshape(4, J, nk)[:, ORDER]
    t[:, 0, :, :nk] = c
    t[:, 1, :, :nk] = s
    t[:, 0, :, nk : 2 * nk] = -s
    t[:, 1, :, nk : 2 * nk] = c
    return np_bf16(t.reshape(4 * LANES, LANES))


def step_tables():
    nk = NCH + 2
    w = np.zeros((NCH // 2, 256, 2, 2, J))
    i = ORDER[:, None]
    j = ORDER[None, :]
    delta = j - i
    ham = (0.54 - 0.46 * np.cos(TH * delta)) / math.sqrt(K) * (delta > 0)
    jj = ORDER
    for k in range(NCH):
        kp, kk = divmod(k, 2)
        gr = ham * np.cos(TH * k * delta)
        gi = ham * np.sin(TH * k * delta)
        w[kp, :J, kk, 0] = gr
        w[kp, :J, kk, 1] = gi
        w[kp, J : 2 * J, kk, 0] = -gi
        w[kp, J : 2 * J, kk, 1] = gr
        for off, coef in ((-1, -0.23), (0, 0.54), (1, -0.23)):
            kap = k + off
            co = coef / math.sqrt(K)
            row = LANES + kap + 1
            w[kp, row, kk, 0] = co * np.cos(TH * kap * jj)
            w[kp, row, kk, 1] = co * np.sin(TH * kap * jj)
            w[kp, row + nk, kk, 0] = -co * np.sin(TH * kap * jj)
            w[kp, row + nk, kk, 1] = co * np.cos(TH * kap * jj)
    return np_bf16(w.reshape(NCH // 2, 256, 256))


def dft_tables():
    group = np.arange(2 * NB * LANES // 2) // 16
    tile, part = group // 8, group % 8
    blk = np.zeros(LB, np.int64)
    low = np.zeros(LB, np.int64)
    for n in range(LB):
        t, q = tile[n], part[n]
        bits = [q % 2, q // 2 % 2]
        low[n] = (t % 2) + 2 * (t // 2 % 2)
        src = (t // 4) * 4 + bits[0] + 2 * bits[1]
        blk[n] = 2 * src + q // 4
    b = blk * J + (np.arange(LB) % 16) * 4 + low
    m = np.arange(LB // 4)
    out = np.zeros((4, 2, LB // 4, 2, LB // 4))
    for r in range(4):
        rows = b[low == r]
        ang = 2.0 * math.pi * ((rows[:, None] * m[None, :]) % LB) / LB
        c, d = np.cos(ang) / math.sqrt(LB), np.sin(ang) / math.sqrt(LB)
        out[r, 0, :, 0] = c
        out[r, 0, :, 1] = -d
        out[r, 1, :, 0] = d
        out[r, 1, :, 1] = c
    return np_bf16(out.reshape(4, LB // 2, LB // 2))


def phase_tables():
    lane = np.arange(LANES)
    left = lane < J
    place = ORDER[lane % J]
    ids = np.arange(16)
    ang = 2.0 * math.pi * ((ids[:, None] * place[None, :]) % 16) / 16
    mod = np.zeros((16, 8, LANES), np.float32)
    mod[:, 0] = np.cos(ang)
    mod[:, 1] = np.where(left, np.sin(ang), -np.sin(ang))
    ang = 2.0 * math.pi * ids[:, None] * place[None, :] / L
    turn = np.zeros((16, 8, LANES), np.float32)
    turn[:, 0] = 0.25 * np.cos(ang)
    turn[:, 1] = 0.25 * np.sin(ang)
    turn[:, 2] = 0.25 * np.where(left, -np.cos(ang), np.cos(ang))
    turn[:, 3] = 0.25 * np.where(left, -np.sin(ang), np.sin(ang))
    ang = np.broadcast_to(2.0 * math.pi * np.arange(K)[:, None] / K, (K, LANES))
    circle = np.stack([np.cos(ang), np.sin(ang)]).astype(np.float32)
    return mod, turn, circle


def pick_table():
    t = np.zeros((2, 2, J, 2, 2, J))
    for lane, j in enumerate(ORDER):
        for c in range(2):
            for e in range(2):
                t[c, e, j, e, c, lane] = 1
    return np_bf16(t.reshape(256, 256))


def swap(x):
    return pltpu.roll(x, J, 1)


MESH = pl.DeviceIdType.MESH


def exchange_parts(g, sems):
    (ts, tr_, xs, xr, rs, rr, ls, lr, ds, dr) = sems
    t = lax.axis_index("tm")
    s = lax.axis_index("strip")
    core = t % 2
    q = t // 2
    z = s // 2
    sib = t + 1 - 2 * core
    other = s + 1 - 2 * (s % 2)
    up = 2 * ((z + 1) % NZ) + s % 2
    down = 2 * ((z + NZ - 1) % NZ) + s % 2

    def peer(d):
        return 2 * ((q + d) % NQ) + core

    def ring(z_from, e, h, right):
        ref = g.at[2 * z_from + e, core]
        send, recv = (rs, rr) if right else (ls, lr)
        return pltpu.make_async_remote_copy(
            src_ref=ref,
            dst_ref=ref,
            send_sem=send.at[h, e],
            recv_sem=recv.at[h, e],
            device_id={"strip": up if right else down},
            device_id_type=MESH,
        )

    def twin(strip, half, slot):
        ref = g.at[strip, half]
        return pltpu.make_async_remote_copy(
            src_ref=ref,
            dst_ref=ref,
            send_sem=ds.at[slot],
            recv_sem=dr.at[slot],
            device_id={"tm": sib},
            device_id_type=MESH,
        )

    def near(d, pos):
        ref = g.at[s, core, pos]
        return pltpu.make_async_remote_copy(
            src_ref=ref,
            dst_ref=ref,
            send_sem=ts.at[d],
            recv_sem=tr_.at[d],
            device_id={"tm": peer(d)},
            device_id_type=MESH,
        )

    def cross(d, strip, pos):
        ref = g.at[strip, core, pos]
        return pltpu.make_async_remote_copy(
            src_ref=ref,
            dst_ref=ref,
            send_sem=xs.at[d],
            recv_sem=xr.at[d],
            device_id={"strip": other, "tm": peer(d)},
            device_id_type=MESH,
        )

    def slot_of(e, h, right):
        return 2 + (h * 2 + e) * 2 + (0 if right else 1)

    def greet():
        barrier = pltpu.get_barrier_semaphore()
        ids = [{"tm": peer(d)} for d in range(1, NQ)]
        ids += [{"strip": other, "tm": peer(d)} for d in range(NQ)]
        ids += [{"tm": sib}, {"strip": up}, {"strip": down}]
        for to in ids:
            pl.semaphore_signal(barrier, inc=1, device_id=to, device_id_type=MESH)

    def begin(piece):
        g[s, core, q] = piece
        barrier = pltpu.get_barrier_semaphore()
        pl.semaphore_wait(barrier, 2 * NQ + 2)
        for d in range(NQ):
            cross(d, s, q).start()
            if d:
                near(d, q).start()

    def joined():
        for d in range(1, NQ):
            near(d, (q + NQ - d) % NQ).wait_recv()
        ring(z, s % 2, 1, True).start()
        ring(z, s % 2, 1, False).start()
        twin(s, core, 0).start()
        for d in range(NQ):
            cross(d, other, (q + NQ - d) % NQ).wait_recv()
        twin(other, core, 1).start()
        ring(z, other % 2, 1, True).start()
        ring(z, other % 2, 1, False).start()
        twin(s, 1 - core, 0).wait_recv()
        twin(other, 1 - core, 1).wait_recv()

    def arrive(h, e, right, last=False):
        zf = (z + NZ - h) % NZ if right else (z + h) % NZ
        ring(zf, e, h, right).wait_recv()
        twin(2 * zf + e, core, slot_of(e, h, right)).start()

        if not last:
            if e == (0 if right else 1):
                ring(zf, e, h + 1, right).start()
            else:

                @pl.when(h < 3)
                def _():
                    ring(zf, e, h + 1, right).start()

    def settle(h, e, right):
        zf = (z + NZ - h) % NZ if right else (z + h) % NZ
        twin(2 * zf + e, 1 - core, slot_of(e, h, right)).wait_recv()

    def close():
        for d in range(NQ):
            cross(d, s, q).wait_send()
            if d:
                near(d, q).wait_send()
        twin(s, core, 0).wait_send()
        twin(other, core, 1).wait_send()
        for right in (True, False):
            for h in range(1, 5):
                for e in range(2):
                    if h == 4 and e != (0 if right else 1):
                        continue
                    zs = (z + NZ - h + 1) % NZ if right else (z + h - 1) % NZ
                    zf = (z + NZ - h) % NZ if right else (z + h) % NZ
                    ring(zs, e, h, right).wait_send()
                    twin(2 * zf + e, core, slot_of(e, h, right)).wait_send()

    return z, greet, begin, joined, arrive, settle, close


def cut(x, pick):
    x = x.astype(F32)
    rows = []
    for n in range(NB // 2):
        both = jnp.concatenate([x[c][:, n * LANES : (n + 1) * LANES] for c in range(2)], axis=1)
        rows += [both, both]
    out = jnp.dot(jnp.concatenate(rows, axis=0).astype(BF16), pick, preferred_element_type=F32)
    low = lax.broadcasted_iota(jnp.int32, (4 * NB, LANES), 0) % 8 < 4
    return jnp.where(low, out[:, :LANES], out[:, LANES:]).astype(BF16)


def body(sig_h, pick_h, mod_h, turn_h, circle_h, tr_h, wt_h, sr_h, si_h, g, sig, pick, mod, turn, circle, tr, wt, pce, pse, y32, yb, lhs, va, vb, sr, si, fl, tab, *sems):
    z0, greet, begin, joined, arrive, settle, close = exchange_parts(g, sems)
    pairs = ((sig_h, sig), (pick_h, pick), (mod_h.at[lax.axis_index("strip")], mod), (turn_h.at[lax.axis_index("tm")], turn), (circle_h, circle), (tr_h, tr), (wt_h, wt))
    tables = [pltpu.make_async_copy(h, v, tab.at[i]) for i, (h, v) in enumerate(pairs)]
    for c in tables:
        c.start()
    greet()
    tables[0].wait()
    tables[1].wait()
    begin(cut(sig[...], pick[...]))
    left = lax.broadcasted_iota(jnp.int32, (1, LANES), 1) < J
    sign = jnp.where(left, -1.0, 1.0).astype(F32)
    rows_all = NA * NB * GW
    for c in tables[2:5]:
        c.wait()
    mc = mod[0:1, :]
    ms = mod[1:2, :]

    me = lax.axis_index("tm")
    turns = [jnp.broadcast_to(turn[i : i + 1, :], (GW, LANES)) for i in range(4)]

    def spread(rho, carry):
        at = (me * rho) % K
        ca = jnp.broadcast_to(circle[0, pl.ds(at, 1), :], (GW, LANES))
        sa = jnp.broadcast_to(circle[1, pl.ds(at, 1), :], (GW, LANES))
        dst = pl.ds(pl.multiple_of(rho * GW, GW), GW)
        pce[dst, :] = ca * turns[0] - sa * turns[1]
        pse[dst, :] = sa * turns[2] + ca * turns[3]
        return carry

    lax.fori_loop(0, NA * NB, spread, 0, unroll=8)
    y32[pl.ds(rows_all, 4 * GW), :] = jnp.zeros((4 * GW, LANES), F32)
    yb[pl.ds(rows_all, 4 * GW), :] = jnp.zeros((4 * GW, LANES), BF16)

    for c in tables[5:]:
        c.wait()
    joined()

    def flush(z):
        return [pltpu.make_async_copy(v.at[:, z], h.at[:, z], fl.at[z, n]) for n, (v, h) in enumerate(((sr, sr_h), (si, si_h)))]

    def group(i, carry):
        half = (i + 1) // 2
        z = (z0 + NZ + half * (1 - 2 * (i % 2))) % NZ

        @pl.when(i % 2 == 1)
        def _():
            @pl.when(half < 4)
            def _():
                for e in range(2):
                    for right in (True, False):
                        arrive(half, e, right)
                for e in range(2):
                    settle(half, e, True)

            @pl.when(half == 4)
            def _():
                arrive(half, 0, True, True)
                arrive(half, 1, False, True)
                settle(half, 0, True)
                settle(half, 1, False)

        @pl.when((i % 2 == 0) & (i > 0))
        def _():
            for e in range(2):
                settle(half, e, False)

        low = lax.broadcasted_iota(jnp.int32, (1, GW, LANES), 1) < 4

        def load_windows(a, c2):
            y = []
            for xh in range(2):
                x = g[2 * z + xh, a % 2, a // 2].astype(F32)
                y.append((x * mc + swap(x) * ms).reshape(NB // 2, GW, LANES))
            even = jnp.where(low, y[0], pltpu.roll(y[1], 4, 1))
            odd = jnp.where(low, pltpu.roll(y[0], 4, 1), y[1])
            both = jnp.stack([even, odd], axis=1).reshape(NB * GW, LANES)
            y32[pl.ds(pl.multiple_of(a * (NB * GW), NB * GW), NB * GW), :] = both
            return c2

        lax.fori_loop(0, NA, load_windows, 0, unroll=16)

        step = 512
        count = rows_all // step
        for i in range(count + 1):
            if i < count:
                r0 = i * step
                rows = slice(r0, r0 + step)
                y = y32[rows, :]
                yb[rows, :] = y.astype(BF16)
                d = y32[r0 + 4 * GW : r0 + 4 * GW + step, :] - y
                lhs[rows, 0:LANES] = d.astype(BF16)
                y2 = y32[r0 + 2 * GW : r0 + 2 * GW + step, :]
                v = y2 * pce[rows, :] + swap(y2) * pse[rows, :]
                va[rows, :] = v
                vb[rows, :] = swap(v) * sign
            if i > 0:
                r0 = (i - 1) * step
                rows = jnp.concatenate([yb[r0 + q * GW : r0 + q * GW + step, :] for q in range(4)], axis=1)
                base = jnp.dot(rows, tr[...], preferred_element_type=F32)
                lhs[r0 : r0 + step, LANES:] = base.astype(BF16)

        def chan_step(kp, c2):
            w = wt[kp]
            for qb in range(NB // QB):
                cuts = [slice((a * NB + qb * QB) * GW, (a * NB + (qb + 1) * QB) * GW) for a in range(NA)]
                x = jnp.dot(
                    jnp.concatenate([lhs[c, :] for c in cuts], axis=0), w, preferred_element_type=F32
                )
                n = QB * GW
                ta = [None] * 2
                tb = [None] * 2
                for a in range(NA):
                    ua = va[cuts[a], :]
                    ub = vb[cuts[a], :]
                    for kk in range(2):
                        xa = x[a * n : (a + 1) * n, kk * LANES : (kk + 1) * LANES]
                        ta[kk] = xa * ua if a == 0 else ta[kk] + xa * ua
                        tb[kk] = xa * ub if a == 0 else tb[kk] + xa * ub
                for kk in range(2):
                    for t, dst in ((ta[kk], sr), (tb[kk], si)):
                        t = t + swap(t)
                        for h in range(QB // 2):
                            even = t[2 * h * GW : (2 * h + 1) * GW]
                            odd = t[(2 * h + 1) * GW : (2 * h + 2) * GW]
                            lane0 = (qb * QB // 2 + h) * LANES
                            dst[2 * kp + kk, z, :, lane0 : lane0 + LANES] = jnp.where(left, even, odd).astype(BF16)
            return c2

        lax.fori_loop(0, NCH // 2, chan_step, 0, unroll=8)
        for c in flush(z):
            c.start()
        return carry

    lax.fori_loop(0, NW // GW, group, 0)
    for z in range(NZ):
        for c in flush(z):
            c.wait()

    close()


def last_pass(sr, si, tab, out, acc):
    lane = lax.broadcasted_iota(jnp.int32, (1, LANES), 1)
    n = KB * NW

    def regroup(ref):
        t = [ref[:, :, :, i * LANES : (i + 1) * LANES].reshape(n, LANES) for i in range(8)]
        for bit in range(2):
            sh = 16 << bit
            low = (lane // sh) % 2 == 0
            for i in range(8):
                if i >> bit & 1:
                    continue
                p, q = t[i], t[i + (1 << bit)]
                t[i] = jnp.where(low, p, pltpu.roll(q, sh, 1))
                t[i + (1 << bit)] = jnp.where(low, pltpu.roll(p, LANES - sh, 1), q)
        return t

    re = regroup(sr)
    im = regroup(si)
    for r in range(4):
        rows = jnp.concatenate([re[r], re[r + 4], im[r], im[r + 4]], axis=1)
        acc[r] = jnp.dot(rows, tab[r], preferred_element_type=F32)
    h = LB // 4
    for c0 in range(0, h, LANES):
        y = [(acc[r, :, c0 : c0 + LANES], acc[r, :, h + c0 : h + c0 + LANES]) for r in range(4)]
        for c in range(2):
            o = 1 - c
            sg = 1.0 if c == 0 else -1.0
            e0 = y[0][c] + y[2][c]
            e1 = y[0][c] - y[2][c]
            o0 = y[1][c] + y[3][c]
            o1 = (y[1][o] - y[3][o]) * sg
            for m1, val in enumerate((e0 + o0, e1 + o1, e0 - o0, e1 - o1)):
                lane0 = m1 * h + c0
                out[c, :, :, lane0 : lane0 + LANES] = val.astype(BF16).reshape(KB, NW, LANES)


def finish(sr, si):
    part = pl.BlockSpec((KB, NW // GW, GW, LB), lambda k: (k, 0, 0, 0))
    return pl.pallas_call(
        last_pass,
        grid=(NCH // KB,),
        out_shape=jax.ShapeDtypeStruct((2, NCH, NW, LB), BF16),
        in_specs=[part, part, pl.BlockSpec((4, LB // 2, LB // 2), lambda k: (0, 0, 0))],
        out_specs=pl.BlockSpec((2, KB, NW, LB), lambda k: (0, k, 0, 0)),
        scratch_shapes=[pltpu.VMEM((4, KB * NW, LB // 2), F32)],
        compiler_params=pltpu.CompilerParams(vmem_limit_bytes=67043328),
    )(sr, si, jnp.asarray(dft_tables()))


def compute(signal):
    hbm = pl.BlockSpec(memory_space=pltpu.HBM)
    dma = pltpu.SemaphoreType.DMA
    rows = NA * NB * GW
    mod, turn, circle = phase_tables()
    strip = jax.ShapeDtypeStruct((NCH, NW // GW, GW, LB), BF16)
    return pl.pallas_call(
        body,
        out_shape=(strip, strip),
        in_specs=[hbm] * 7,
        out_specs=(hbm, hbm),
        scratch_shapes=[
            pltpu.VMEM((2 * NZ, 2, NQ, 4 * NB, LANES), BF16),
            pltpu.VMEM((2, 4, LB), BF16),
            pltpu.VMEM((256, 256), BF16),
            pltpu.VMEM((8, LANES), F32),
            pltpu.VMEM((8, LANES), F32),
            pltpu.VMEM((2, K, LANES), F32),
            pltpu.VMEM((4 * LANES, LANES), BF16),
            pltpu.VMEM((NCH // 2, 256, 256), BF16),
            pltpu.VMEM((rows, LANES), F32),
            pltpu.VMEM((rows, LANES), F32),
            pltpu.VMEM((rows + 4 * GW, LANES), F32),
            pltpu.VMEM((rows + 4 * GW, LANES), BF16),
            pltpu.VMEM((rows, 256), BF16),
            pltpu.VMEM((rows, LANES), F32),
            pltpu.VMEM((rows, LANES), F32),
            pltpu.VMEM((NCH, NW // GW, GW, LB), BF16),
            pltpu.VMEM((NCH, NW // GW, GW, LB), BF16),
            dma((NZ, 2)),
            dma((7,)),
            dma((NQ,)),
            dma((NQ,)),
            dma((NQ,)),
            dma((NQ,)),
            dma((5, 2)),
            dma((5, 2)),
            dma((5, 2)),
            dma((5, 2)),
            dma((22,)),
            dma((22,)),
        ],
        compiler_params=pltpu.CompilerParams(
            vmem_limit_bytes=67043328, collective_id=0, has_side_effects=True
        ),
    )(signal, jnp.asarray(pick_table()), jnp.asarray(mod), jnp.asarray(turn), jnp.asarray(circle), jnp.asarray(base_table()), jnp.asarray(step_tables()))


def per_device(signal):
    sr, si = compute(signal)
    return finish(sr, si).reshape(2, NCH, NW, 1, LB)


def solution(mesh):
    return jax.shard_map(
        per_device,
        mesh=mesh,
        in_specs=(P(None, "strip", "tm"),),
        out_specs=P(None, "strip", None, "tm", None),
        check_vma=False,
    )
```

```python
import math

import jax
import jax.numpy as jnp
import numpy as np
from jax import lax
from jax.experimental import pallas as pl
from jax.experimental.pallas import tpu as pltpu
from jax.sharding import PartitionSpec as P

K = 256
J = 64
L = 16384
NB = 16
NA = 16
NW = 64
LB = 1024
NCH = 16
LANES = 128
GW = 8
NZ = 8
NQ = 8
KB = 8
LIM1 = 60600000
LIM2 = 40 * 2**20
QB = 4
TH = 2.0 * math.pi / K
F32 = jnp.float32
BF16 = jnp.bfloat16


ORDER = np.arange(J).reshape(J // 4, 4).T.reshape(J)


def np_bf16(x):
    return np.asarray(x, np.float32).astype(jnp.bfloat16)


def base_table():
    kap = np.arange(-1, NCH + 1)
    r = np.arange(K)
    ang = TH * ((r[:, None] * kap[None, :]) % K)
    c, s = np.cos(ang), np.sin(ang)
    t = np.zeros((4, 2, J, LANES))
    nk = NCH + 2
    c = c.reshape(4, J, nk)[:, ORDER]
    s = s.reshape(4, J, nk)[:, ORDER]
    t[:, 0, :, :nk] = c
    t[:, 1, :, :nk] = s
    t[:, 0, :, nk : 2 * nk] = -s
    t[:, 1, :, nk : 2 * nk] = c
    return np_bf16(t.reshape(4 * LANES, LANES))


def step_tables():
    nk = NCH + 2
    w = np.zeros((NCH // 2, 256, 2, 2, J))
    i = ORDER[:, None]
    j = ORDER[None, :]
    delta = j - i
    ham = (0.54 - 0.46 * np.cos(TH * delta)) / math.sqrt(K) * (delta > 0)
    jj = ORDER
    for k in range(NCH):
        kp, kk = divmod(k, 2)
        gr = ham * np.cos(TH * k * delta)
        gi = ham * np.sin(TH * k * delta)
        w[kp, :J, kk, 0] = gr
        w[kp, :J, kk, 1] = gi
        w[kp, J : 2 * J, kk, 0] = -gi
        w[kp, J : 2 * J, kk, 1] = gr
        for off, coef in ((-1, -0.23), (0, 0.54), (1, -0.23)):
            kap = k + off
            co = coef / math.sqrt(K)
            row = LANES + kap + 1
            w[kp, row, kk, 0] = co * np.cos(TH * kap * jj)
            w[kp, row, kk, 1] = co * np.sin(TH * kap * jj)
            w[kp, row + nk, kk, 0] = -co * np.sin(TH * kap * jj)
            w[kp, row + nk, kk, 1] = co * np.cos(TH * kap * jj)
    return np_bf16(w.reshape(NCH // 2, 256, 256))


def dft_tables():
    group = np.arange(2 * NB * LANES // 2) // 16
    tile, part = group // 8, group % 8
    blk = np.zeros(LB, np.int64)
    low = np.zeros(LB, np.int64)
    for n in range(LB):
        t, q = tile[n], part[n]
        bits = [q % 2, q // 2 % 2]
        low[n] = (t % 2) + 2 * (t // 2 % 2)
        src = (t // 4) * 4 + bits[0] + 2 * bits[1]
        blk[n] = 2 * src + q // 4
    b = blk * J + (np.arange(LB) % 16) * 4 + low
    m = np.arange(LB // 4)
    out = np.zeros((4, 2, LB // 4, 2, LB // 4))
    for r in range(4):
        rows = b[low == r]
        ang = 2.0 * math.pi * ((rows[:, None] * m[None, :]) % LB) / LB
        c, d = np.cos(ang) / math.sqrt(LB), np.sin(ang) / math.sqrt(LB)
        out[r, 0, :, 0] = c
        out[r, 0, :, 1] = -d
        out[r, 1, :, 0] = d
        out[r, 1, :, 1] = c
    return np_bf16(out.reshape(4, LB // 2, LB // 2))


def phase_tables():
    lane = np.arange(LANES)
    left = lane < J
    place = ORDER[lane % J]
    ids = np.arange(16)
    ang = 2.0 * math.pi * ((ids[:, None] * place[None, :]) % 16) / 16
    mod = np.zeros((16, 8, LANES), np.float32)
    mod[:, 0] = np.cos(ang)
    mod[:, 1] = np.where(left, np.sin(ang), -np.sin(ang))
    ang = 2.0 * math.pi * ids[:, None] * place[None, :] / L
    turn = np.zeros((16, 8, LANES), np.float32)
    turn[:, 0] = 0.25 * np.cos(ang)
    turn[:, 1] = 0.25 * np.sin(ang)
    turn[:, 2] = 0.25 * np.where(left, -np.cos(ang), np.cos(ang))
    turn[:, 3] = 0.25 * np.where(left, -np.sin(ang), np.sin(ang))
    ang = np.broadcast_to(2.0 * math.pi * np.arange(K)[:, None] / K, (K, LANES))
    circle = np.stack([np.cos(ang), np.sin(ang)]).astype(np.float32)
    return mod, turn, circle


def pick_table():
    t = np.zeros((2, 2, J, 2, 2, J))
    for lane, j in enumerate(ORDER):
        for c in range(2):
            for e in range(2):
                t[c, e, j, e, c, lane] = 1
    return np_bf16(t.reshape(256, 256))


def swap(x):
    return pltpu.roll(x, J, 1)


MESH = pl.DeviceIdType.MESH


def exchange_parts(g, sems):
    (ts, tr_, xs, xr, rs, rr, ls, lr, ds, dr) = sems
    t = lax.axis_index("tm")
    s = lax.axis_index("strip")
    core = t % 2
    q = t // 2
    z = s // 2
    sib = t + 1 - 2 * core
    other = s + 1 - 2 * (s % 2)
    up = 2 * ((z + 1) % NZ) + s % 2
    down = 2 * ((z + NZ - 1) % NZ) + s % 2

    def peer(d):
        return 2 * ((q + d) % NQ) + core

    def ring(z_from, e, h, right):
        ref = g.at[2 * z_from + e, core]
        send, recv = (rs, rr) if right else (ls, lr)
        return pltpu.make_async_remote_copy(
            src_ref=ref,
            dst_ref=ref,
            send_sem=send.at[h, e],
            recv_sem=recv.at[h, e],
            device_id={"strip": up if right else down},
            device_id_type=MESH,
        )

    def twin(strip, half, slot):
        ref = g.at[strip, half]
        return pltpu.make_async_remote_copy(
            src_ref=ref,
            dst_ref=ref,
            send_sem=ds.at[slot],
            recv_sem=dr.at[slot],
            device_id={"tm": sib},
            device_id_type=MESH,
        )

    def near(d, pos):
        ref = g.at[s, core, pos]
        return pltpu.make_async_remote_copy(
            src_ref=ref,
            dst_ref=ref,
            send_sem=ts.at[d],
            recv_sem=tr_.at[d],
            device_id={"tm": peer(d)},
            device_id_type=MESH,
        )

    def cross(d, strip, pos):
        ref = g.at[strip, core, pos]
        return pltpu.make_async_remote_copy(
            src_ref=ref,
            dst_ref=ref,
            send_sem=xs.at[d],
            recv_sem=xr.at[d],
            device_id={"strip": other, "tm": peer(d)},
            device_id_type=MESH,
        )

    def slot_of(e, h, right):
        return 2 + (h * 2 + e) * 2 + (0 if right else 1)

    def greet():
        barrier = pltpu.get_barrier_semaphore()
        ids = [{"tm": peer(d)} for d in range(1, NQ)]
        ids += [{"strip": other, "tm": peer(d)} for d in range(NQ)]
        ids += [{"tm": sib}, {"strip": up}, {"strip": down}]
        for to in ids:
            pl.semaphore_signal(barrier, inc=1, device_id=to, device_id_type=MESH)

    def begin(piece):
        g[s, core, q] = piece
        barrier = pltpu.get_barrier_semaphore()
        pl.semaphore_wait(barrier, 2 * NQ + 2)
        for d in range(NQ):
            cross(d, s, q).start()
            if d:
                near(d, q).start()

    def joined():
        for d in range(1, NQ):
            near(d, (q + NQ - d) % NQ).wait_recv()
        ring(z, s % 2, 1, True).start()
        ring(z, s % 2, 1, False).start()
        twin(s, core, 0).start()
        for d in range(NQ):
            cross(d, other, (q + NQ - d) % NQ).wait_recv()
        twin(other, core, 1).start()
        ring(z, other % 2, 1, True).start()
        ring(z, other % 2, 1, False).start()
        twin(s, 1 - core, 0).wait_recv()
        twin(other, 1 - core, 1).wait_recv()

    def arrive(h, e, right, last=False):
        zf = (z + NZ - h) % NZ if right else (z + h) % NZ
        ring(zf, e, h, right).wait_recv()
        twin(2 * zf + e, core, slot_of(e, h, right)).start()

        if not last:
            if e == (0 if right else 1):
                ring(zf, e, h + 1, right).start()
            else:

                @pl.when(h < 3)
                def _():
                    ring(zf, e, h + 1, right).start()

    def settle(h, e, right):
        zf = (z + NZ - h) % NZ if right else (z + h) % NZ
        twin(2 * zf + e, 1 - core, slot_of(e, h, right)).wait_recv()

    def close():
        for d in range(NQ):
            cross(d, s, q).wait_send()
            if d:
                near(d, q).wait_send()
        twin(s, core, 0).wait_send()
        twin(other, core, 1).wait_send()
        for right in (True, False):
            for h in range(1, 5):
                for e in range(2):
                    if h == 4 and e != (0 if right else 1):
                        continue
                    zs = (z + NZ - h + 1) % NZ if right else (z + h - 1) % NZ
                    zf = (z + NZ - h) % NZ if right else (z + h) % NZ
                    ring(zs, e, h, right).wait_send()
                    twin(2 * zf + e, core, slot_of(e, h, right)).wait_send()

    return z, greet, begin, joined, arrive, settle, close


def cut(x, pick):
    x = x.astype(F32)
    rows = []
    for n in range(NB // 2):
        both = jnp.concatenate([x[c][:, n * LANES : (n + 1) * LANES] for c in range(2)], axis=1)
        rows += [both, both]
    out = jnp.dot(jnp.concatenate(rows, axis=0).astype(BF16), pick, preferred_element_type=F32)
    low = lax.broadcasted_iota(jnp.int32, (4 * NB, LANES), 0) % 8 < 4
    return jnp.where(low, out[:, :LANES], out[:, LANES:]).astype(BF16)


def body(sig_h, pick_h, mod_h, turn_h, circle_h, tr_h, wt_h, dft_h, sr, si, dft, g, sig, pick, mod, turn, circle, tr, wt, pce, pse, y32, yb, lhs, va, vb, tab, *sems):
    z0, greet, begin, joined, arrive, settle, close = exchange_parts(g, sems)
    pairs = ((sig_h, sig), (pick_h, pick), (mod_h.at[lax.axis_index("strip")], mod), (turn_h.at[lax.axis_index("tm")], turn), (circle_h, circle), (tr_h, tr), (wt_h, wt), (dft_h, dft))
    tables = [pltpu.make_async_copy(h, v, tab.at[i]) for i, (h, v) in enumerate(pairs)]
    for c in tables[:2]:
        c.start()
    greet()
    for c in tables[2:]:
        c.start()
    tables[0].wait()
    tables[1].wait()
    begin(cut(sig[...], pick[...]))
    left = lax.broadcasted_iota(jnp.int32, (1, LANES), 1) < J
    sign = jnp.where(left, -1.0, 1.0).astype(F32)
    rows_all = NA * NB * GW
    for c in tables[2:5]:
        c.wait()
    mc = mod[0:1, :]
    ms = mod[1:2, :]

    me = lax.axis_index("tm")
    turns = [jnp.broadcast_to(turn[i : i + 1, :], (GW, LANES)) for i in range(4)]

    def spread(rho, carry):
        at = (me * rho) % K
        ca = jnp.broadcast_to(circle[0, pl.ds(at, 1), :], (GW, LANES))
        sa = jnp.broadcast_to(circle[1, pl.ds(at, 1), :], (GW, LANES))
        dst = pl.ds(pl.multiple_of(rho * GW, GW), GW)
        pce[dst, :] = ca * turns[0] - sa * turns[1]
        pse[dst, :] = sa * turns[2] + ca * turns[3]
        return carry

    lax.fori_loop(0, NA * NB, spread, 0, unroll=8)
    y32[pl.ds(rows_all, 4 * GW), :] = jnp.zeros((4 * GW, LANES), F32)
    yb[pl.ds(rows_all, 4 * GW), :] = jnp.zeros((4 * GW, LANES), BF16)

    for c in tables[5:7]:
        c.wait()
    joined()

    def group(i, carry):
        half = (i + 1) // 2
        z = (z0 + NZ + half * (1 - 2 * (i % 2))) % NZ

        @pl.when(i % 2 == 1)
        def _():
            @pl.when(half < 4)
            def _():
                for e in range(2):
                    for right in (True, False):
                        arrive(half, e, right)
                for e in range(2):
                    settle(half, e, True)

            @pl.when(half == 4)
            def _():
                arrive(half, 0, True, True)
                arrive(half, 1, False, True)
                settle(half, 0, True)
                settle(half, 1, False)

        @pl.when((i % 2 == 0) & (i > 0))
        def _():
            for e in range(2):
                settle(half, e, False)

        low = lax.broadcasted_iota(jnp.int32, (1, GW, LANES), 1) < 4

        def load_windows(a, c2):
            y = []
            for xh in range(2):
                x = g[2 * z + xh, a % 2, a // 2].astype(F32)
                y.append((x * mc + swap(x) * ms).reshape(NB // 2, GW, LANES))
            even = jnp.where(low, y[0], pltpu.roll(y[1], 4, 1))
            odd = jnp.where(low, pltpu.roll(y[0], 4, 1), y[1])
            both = jnp.stack([even, odd], axis=1).reshape(NB * GW, LANES)
            y32[pl.ds(pl.multiple_of(a * (NB * GW), NB * GW), NB * GW), :] = both
            return c2

        lax.fori_loop(0, NA, load_windows, 0, unroll=16)

        step = 512
        count = rows_all // step
        for i in range(count + 1):
            if i < count:
                r0 = i * step
                rows = slice(r0, r0 + step)
                y = y32[rows, :]
                yb[rows, :] = y.astype(BF16)
                d = y32[r0 + 4 * GW : r0 + 4 * GW + step, :] - y
                lhs[rows, 0:LANES] = d.astype(BF16)
                y2 = y32[r0 + 2 * GW : r0 + 2 * GW + step, :]
                v = y2 * pce[rows, :] + swap(y2) * pse[rows, :]
                va[rows, :] = v
                vb[rows, :] = swap(v) * sign
            if i > 0:
                r0 = (i - 1) * step
                rows = jnp.concatenate([yb[r0 + q * GW : r0 + q * GW + step, :] for q in range(4)], axis=1)
                base = jnp.dot(rows, tr[...], preferred_element_type=F32)
                lhs[r0 : r0 + step, LANES:] = base.astype(BF16)

        def chan_step(kp, c2):
            w = wt[kp]
            for qb in range(NB // QB):
                cuts = [slice((a * NB + qb * QB) * GW, (a * NB + (qb + 1) * QB) * GW) for a in range(NA)]
                x = jnp.dot(
                    jnp.concatenate([lhs[c, :] for c in cuts], axis=0), w, preferred_element_type=F32
                )
                n = QB * GW
                ta = [None] * 2
                tb = [None] * 2
                for a in range(NA):
                    ua = va[cuts[a], :]
                    ub = vb[cuts[a], :]
                    for kk in range(2):
                        xa = x[a * n : (a + 1) * n, kk * LANES : (kk + 1) * LANES]
                        ta[kk] = xa * ua if a == 0 else ta[kk] + xa * ua
                        tb[kk] = xa * ub if a == 0 else tb[kk] + xa * ub
                for kk in range(2):
                    for t, dst in ((ta[kk], sr), (tb[kk], si)):
                        t = t + swap(t)
                        for h in range(QB // 2):
                            even = t[2 * h * GW : (2 * h + 1) * GW]
                            odd = t[(2 * h + 1) * GW : (2 * h + 2) * GW]
                            lane0 = (qb * QB // 2 + h) * LANES
                            dst[2 * kp + kk, z, :, lane0 : lane0 + LANES] = jnp.where(left, even, odd).astype(BF16)
            return c2

        lax.fori_loop(0, NCH // 2, chan_step, 0, unroll=8)
        return carry

    lax.fori_loop(0, NW // GW, group, 0)

    tables[7].wait()
    close()


def last_pass(sr, si, tab, out, acc):
    lane = lax.broadcasted_iota(jnp.int32, (1, LANES), 1)
    n = KB * NW
    mine = pl.ds(pl.program_id(0) * KB, KB)

    def regroup(ref):
        t = [ref[mine, :, :, i * LANES : (i + 1) * LANES].reshape(n, LANES) for i in range(8)]
        for bit in range(2):
            sh = 16 << bit
            low = (lane // sh) % 2 == 0
            for i in range(8):
                if i >> bit & 1:
                    continue
                p, q = t[i], t[i + (1 << bit)]
                t[i] = jnp.where(low, p, pltpu.roll(q, sh, 1))
                t[i + (1 << bit)] = jnp.where(low, pltpu.roll(p, LANES - sh, 1), q)
        return t

    re = regroup(sr)
    im = regroup(si)
    for r in range(4):
        rows = jnp.concatenate([re[r], re[r + 4], im[r], im[r + 4]], axis=1)
        acc[r] = jnp.dot(rows, tab[r], preferred_element_type=F32)
    h = LB // 4
    for c0 in range(0, h, LANES):
        y = [(acc[r, :, c0 : c0 + LANES], acc[r, :, h + c0 : h + c0 + LANES]) for r in range(4)]
        for c in range(2):
            o = 1 - c
            sg = 1.0 if c == 0 else -1.0
            e0 = y[0][c] + y[2][c]
            e1 = y[0][c] - y[2][c]
            o0 = y[1][c] + y[3][c]
            o1 = (y[1][o] - y[3][o]) * sg
            for m1, val in enumerate((e0 + o0, e1 + o1, e0 - o0, e1 - o1)):
                lane0 = m1 * h + c0
                out[c, :, :, lane0 : lane0 + LANES] = val.astype(BF16).reshape(KB, NW, LANES)


def finish(sr, si, tab):
    vm = pl.BlockSpec(memory_space=pltpu.VMEM)
    return pl.pallas_call(
        last_pass,
        grid=(NCH // KB,),
        out_shape=jax.ShapeDtypeStruct((2, NCH, NW, LB), BF16),
        in_specs=[vm, vm, vm],
        out_specs=pl.BlockSpec((2, KB, NW, LB), lambda k: (0, k, 0, 0)),
        scratch_shapes=[pltpu.VMEM((4, KB * NW, LB // 2), F32)],
        compiler_params=pltpu.CompilerParams(vmem_limit_bytes=LIM2),
    )(sr, si, tab)


def compute(signal):
    hbm = pl.BlockSpec(memory_space=pltpu.HBM)
    vm = pl.BlockSpec(memory_space=pltpu.VMEM)
    dma = pltpu.SemaphoreType.DMA
    rows = NA * NB * GW
    mod, turn, circle = phase_tables()
    strip = pltpu.VMEM((NCH, NW // GW, GW, LB), BF16)
    quarter = pltpu.VMEM((4, LB // 2, LB // 2), BF16)
    return pl.pallas_call(
        body,
        out_shape=(strip, strip, quarter),
        in_specs=[hbm] * 8,
        out_specs=(vm, vm, vm),
        scratch_shapes=[
            pltpu.VMEM((2 * NZ, 2, NQ, 4 * NB, LANES), BF16),
            pltpu.VMEM((2, 4, LB), BF16),
            pltpu.VMEM((256, 256), BF16),
            pltpu.VMEM((8, LANES), F32),
            pltpu.VMEM((8, LANES), F32),
            pltpu.VMEM((2, K, LANES), F32),
            pltpu.VMEM((4 * LANES, LANES), BF16),
            pltpu.VMEM((NCH // 2, 256, 256), BF16),
            pltpu.VMEM((rows, LANES), F32),
            pltpu.VMEM((rows, LANES), F32),
            pltpu.VMEM((rows + 4 * GW, LANES), F32),
            pltpu.VMEM((rows + 4 * GW, LANES), BF16),
            pltpu.VMEM((rows, 256), BF16),
            pltpu.VMEM((rows, LANES), F32),
            pltpu.VMEM((rows, LANES), F32),
            dma((8,)),
            dma((NQ,)),
            dma((NQ,)),
            dma((NQ,)),
            dma((NQ,)),
            dma((5, 2)),
            dma((5, 2)),
            dma((5, 2)),
            dma((5, 2)),
            dma((22,)),
            dma((22,)),
        ],
        compiler_params=pltpu.CompilerParams(
            vmem_limit_bytes=LIM1, collective_id=0, has_side_effects=True
        ),
    )(signal, jnp.asarray(pick_table()), jnp.asarray(mod), jnp.asarray(turn), jnp.asarray(circle), jnp.asarray(base_table()), jnp.asarray(step_tables()), jnp.asarray(dft_tables()))


def per_device(signal):
    return finish(*compute(signal)).reshape(2, NCH, NW, 1, LB)


def solution(mesh):
    return jax.shard_map(
        per_device,
        mesh=mesh,
        in_specs=(P(None, "strip", "tm"),),
        out_specs=P(None, "strip", None, "tm", None),
        check_vma=False,
    )
```
